256 devices in a mesh: seq: 32 (over x, z), head: 8 (over y, core).
Axes of the slice: x: 4, y: 4, z: 8, core: 2. Of those that a mesh axis runs over, the one named last changes fastest.
Arguments:
- queries: bfloat16 [32768, 4096], P('seq', 'head'), may hold values from -100 to 100
- keys: bfloat16 [32768, 4096], P('seq', 'head'), may hold values from -8 to 8
- values: bfloat16 [32768, 4096], P('seq', 'head'), may hold values from -6 to 6
- rates: float32 [32768, 16], P('seq', 'head'), may hold values from 0.001 to 0.01
- head_scale: float32 [16], P('head'), may hold values from 0.3 to 3
- w_one: float32 [16, 256, 256], P('head'), may hold values from -0.375 to 0.375
- w_three: float32 [16, 256, 256], P('head'), may hold values from -0.375 to 0.375
- w_two: float32 [16, 256, 256], P('head'), may hold values from -0.375 to 0.375
Outputs:
- mixed: float32 [32768, 4096], P('seq', 'head')
- new_one: float32 [16, 256, 256], P('head')
- new_three: float32 [16, 256, 256], P('head')
- new_two: float32 [16, 256, 256], P('head')
The draws below stay inside these ranges and needn't reach their ends.
All inputs are finite; a program needn't handle non-finite values.
Results may differ from the reference program's by a relative error of at most 0.00065.
Values may be sent and summed in bfloat16 or wider, within the bound.
A program may use at most 64 MiB of HBM per device.

```python
import math
import jax
import jax.numpy as jnp
from jax import lax

HEAD_SIZE = 256
WINDOW_SPAN = 512
HEADS = 16
TOKENS = 32768


def draw_pair(key):
    base = jax.random.fold_in(key, 71)
    shape = (TOKENS, HEADS * HEAD_SIZE)
    key_vals = jnp.clip(jax.random.normal(jax.random.fold_in(base, 1), shape, jnp.float32), -6.0, 6.0)
    query_vals = jnp.clip(jax.random.normal(jax.random.fold_in(base, 2), shape, jnp.float32), -6.0, 6.0)
    return (query_vals, key_vals)


def draw_queries(key, part):
    return draw_pair(key)[0].astype(jnp.bfloat16)


def draw_keys(key, part):
    return draw_pair(key)[1].astype(jnp.bfloat16)


def shard_levels(rng, shape, cuts, low, top_value):
    gain, own = 1.0, jax.random.fold_in(rng, 6)
    for dim, shards_of in cuts:
        heights = jnp.exp(jax.random.uniform(jax.random.fold_in(own, dim), (shards_of,), jnp.float32, low / len(cuts), top_value / len(cuts)))
        gain = gain * jnp.repeat(heights, shape[dim] // shards_of).reshape([-1 if axis == dim else 1 for axis in range(len(shape))])
    return gain


def bell_draw(own_key, extent, spread, reach, shards=(), kind=jnp.bfloat16):
    result = spread * jax.random.normal(own_key, extent, jnp.float32)
    if shards:
        result = result * shard_levels(own_key, extent, shards, -0.22, 0.18)
    return jnp.clip(result, -reach, reach).astype(kind)


def setup_inputs(seed: int = 0) -> dict:
    streams_of = jax.random.split(jax.random.key(seed), 9)
    return {
        "queries": draw_queries(jax.random.fold_in(streams_of[8], 71), 0),
        "keys": draw_keys(jax.random.fold_in(streams_of[8], 71), 0),
        "values": bell_draw(streams_of[2], (TOKENS, HEADS * HEAD_SIZE), 1.0, 6.0, ((0, 32), (1, 8))),
        "rates": jnp.clip(jnp.exp(math.log(0.01) - 2.30258502 * jax.random.uniform(streams_of[3], (TOKENS, HEADS), jnp.float32) ** shard_levels(streams_of[3], (TOKENS, HEADS), ((0, 32), (1, 8)), -0.2, 0.2)), 0.001, 0.01),
        "head_scale": jnp.clip(jnp.exp(math.log(3.0) - 2.3025851 * jax.random.uniform(streams_of[4], (HEADS,), jnp.float32) ** shard_levels(streams_of[4], (HEADS,), ((0, 8),), -0.2, 0.2)), 0.3, 3.0),
        "w_one": bell_draw(streams_of[5], (HEADS, HEAD_SIZE, HEAD_SIZE), HEAD_SIZE ** -0.5, 0.375, ((0, 8),), jnp.float32),
        "w_three": bell_draw(streams_of[6], (HEADS, HEAD_SIZE, HEAD_SIZE), HEAD_SIZE ** -0.5, 0.375, ((0, 8),), jnp.float32),
        "w_two": bell_draw(streams_of[7], (HEADS, HEAD_SIZE, HEAD_SIZE), HEAD_SIZE ** -0.5, 0.375, ((0, 8),), jnp.float32),
    }


HIGH = lax.Precision.HIGHEST
EPS = 1e-06

def renorm(weight, grad):
    upd = weight + grad
    old = jnp.sqrt(lax.optimization_barrier(jnp.sum(weight * weight, axis=0, keepdims=True)) + EPS)
    cur = jnp.sqrt(lax.optimization_barrier(jnp.sum(upd * upd, axis=0, keepdims=True)) + EPS)
    return upd * (old / cur)

def one_head(inputs):
    query, key_rows, value_rows, rate, w1, w3, w2 = inputs
    kf = key_rows.astype(jnp.float32)
    vf = value_rows.astype(jnp.float32)
    qf = query.astype(jnp.float32)
    h1 = jnp.dot(kf, w1, precision=HIGH)
    h3 = jnp.dot(kf, w3, precision=HIGH)
    sg = jax.nn.sigmoid(h1)
    sil = h1 * sg
    act = sil * h3
    scaled = rate[:, None] * vf
    g2 = jnp.dot(act.T, scaled, precision=HIGH)
    dact = jnp.dot(scaled, w2.T, precision=HIGH)
    d1 = dact * h3 * sg * (1.0 + h1 * (1.0 - sg))
    d3 = dact * sil
    g1 = jnp.dot(kf.T, d1, precision=HIGH)
    g3 = jnp.dot(kf.T, d3, precision=HIGH)
    n1 = renorm(w1, g1)
    n3 = renorm(w3, g3)
    n2 = renorm(w2, g2)
    p1 = jnp.dot(qf, n1, precision=HIGH)
    p3 = jnp.dot(qf, n3, precision=HIGH)
    outer = jnp.dot(p1 * jax.nn.sigmoid(p1) * p3, n2, precision=HIGH)
    return (n1, n3, n2, outer)

def reference(queries, keys, values, rates, head_scale, w_one, w_three, w_two):
    total = queries.shape[0]
    head_group = w_one.shape[0]
    span_size = w_one.shape[1]
    qh = queries.reshape(total, head_group, span_size).transpose(1, 0, 2)
    kh = keys.reshape(total, head_group, span_size).transpose(1, 0, 2)
    value_head = values.reshape(total, head_group, span_size).transpose(1, 0, 2)
    n1, n3, n2, outer = lax.map(one_head, (qh, kh, value_head, rates.T, w_one, w_three, w_two))
    zed = outer * head_scale[:, None, None]
    mean_sq = lax.optimization_barrier(jnp.sum(zed * zed, axis=(0, 2))) / (head_group * span_size)
    ynorm = zed / jnp.sqrt(mean_sq + EPS)[None, :, None]
    block_span = min(512, total)
    kpad = jnp.concatenate([jnp.zeros((head_group, WINDOW_SPAN, span_size), jnp.bfloat16), kh], axis=1)
    padded_values = jnp.concatenate([jnp.zeros((head_group, WINDOW_SPAN, span_size), jnp.bfloat16), value_head], axis=1)
    scale = span_size ** (-0.5)

    def attend(index):
        start_offset = (index * block_span).astype(jnp.int32)
        qb = lax.dynamic_slice_in_dim(qh, start_offset, block_span, 1).astype(jnp.float32)
        kb = lax.dynamic_slice_in_dim(kpad, start_offset, block_span + WINDOW_SPAN, 1).astype(jnp.float32)
        value_block = lax.dynamic_slice_in_dim(padded_values, start_offset, block_span + WINDOW_SPAN, 1).astype(jnp.float32)
        scores = jnp.einsum('hid,hjd->hij', qb, kb) * scale
        rows = jnp.arange(block_span, dtype=jnp.int32)[:, None]
        cols = jnp.arange(block_span + WINDOW_SPAN, dtype=jnp.int32)[None, :]
        allowed = (cols > rows) & (cols <= rows + WINDOW_SPAN) & (start_offset + cols - WINDOW_SPAN >= 0)
        scores = jnp.where(allowed[None], scores, -jnp.inf)
        top = lax.optimization_barrier(jnp.max(scores, axis=-1, keepdims=True))
        expo = jnp.exp(scores - top)
        weights = (expo / lax.optimization_barrier(jnp.sum(expo, axis=-1, keepdims=True))).astype(jnp.bfloat16)
        return jnp.einsum('hij,hjd->hid', weights.astype(jnp.float32), value_block)
    attn = lax.map(attend, jnp.arange(total // block_span, dtype=jnp.int32))
    attn = attn.transpose(1, 0, 2, 3).reshape(head_group, total, span_size)
    mixed = (attn + ynorm).transpose(1, 0, 2).reshape(total, head_group * span_size).astype(jnp.float32)
    return (mixed, n1, n3, n2)
```

```python
import jax
import jax.numpy as jnp
from jax import lax
from jax.experimental import pallas as pl
from jax.experimental.pallas import tpu as pltpu
from jax.sharding import PartitionSpec as P

WINDOW = 512
EPS = 1e-06
F32 = jnp.float32
BF16 = jnp.bfloat16
MESH = pl.DeviceIdType.MESH
XS, ZS, HS = 4, 8, 8
TOK, FEAT, BLK = 1024, 256, 256
NT = (((1,), (1,)), ((), ()))
NN = (((1,), (0,)), ((), ()))


def mm(a, b, dims):
    return lax.dot_general(a, b, dims, preferred_element_type=F32)


def split(x):
    hi = x.astype(BF16)
    return hi, (x - hi.astype(F32)).astype(BF16)


def cols(h):
    return pl.ds(h * FEAT, FEAT)


def layer(
    q_hbm, k_hbm, v_hbm, rate_hbm, hscale, w1_hbm, w3_hbm, w2_hbm,
    mixed_hbm, n1_hbm, n3_hbm, n2_hbm,
    q, kx, vx, rate, w, wt, wb, dt, g, rx, sx, rz, nt, nb, nout, z, out, sq,
    in_sem, out_sem, halo_s, halo_r, xs_s, xs_r, zs_s, zs_r, za_s, za_r, xa_s, xa_r, sq_s, sq_r,
):
    s = lax.axis_index("seq")
    me_h = lax.axis_index("head")
    x = s // ZS
    zz = s % ZS

    def x_peer(d):
        return ((x + d) % XS) * ZS + zz

    def z_peer(d):
        return x * ZS + (zz + d) % ZS

    barrier = pltpu.get_barrier_semaphore()
    greeted = 0
    for d in range(1, XS):
        pl.semaphore_signal(barrier, inc=1, device_id={"seq": x_peer(d)}, device_id_type=MESH)
        greeted += 1
    for d in range(1, ZS):
        pl.semaphore_signal(barrier, inc=1, device_id={"seq": z_peer(d)}, device_id_type=MESH)
        greeted += 1
    for d in range(1, HS):
        pl.semaphore_signal(barrier, inc=1, device_id={"head": (me_h + d) % HS}, device_id_type=MESH)
        greeted += 1
    after = (s + 1) % (XS * ZS)
    for peer in (after, (s + XS * ZS - 1) % (XS * ZS)):
        pl.semaphore_signal(barrier, inc=1, device_id={"seq": peer}, device_id_type=MESH)
        greeted += 1

    def fetch(src, dst, i):
        copy = pltpu.make_async_copy(src, dst, in_sem.at[i])
        copy.start()
        return copy

    loads = [
        fetch(k_hbm, kx.at[pl.ds(WINDOW, TOK), :], 0),
        fetch(v_hbm, vx.at[pl.ds(WINDOW, TOK), :], 1),
        fetch(w1_hbm, w.at[0], 2),
        fetch(w3_hbm, w.at[1], 3),
        fetch(w2_hbm, w.at[2], 4),
        fetch(rate_hbm, rate, 5),
        fetch(q_hbm, q, 6),
    ]
    for load in loads[2:5]:
        load.wait()
    for h in range(2):
        for m in range(3):
            wt[h, m] = w[m, h].T
        for m in range(2):
            hi, lo = split(wt[h, m])
            wb[h, m, 0] = hi
            wb[h, m, 1] = lo
        hi, lo = split(w[2, h])
        wb[h, 2, 0] = hi
        wb[h, 2, 1] = lo
    for load in loads[:2] + loads[5:]:
        load.wait()

    def gradients(h):
        @pl.loop(0, TOK // BLK)
        def _(i):
            start = pl.multiple_of(i * BLK, BLK)
            kt = kx[pl.ds(WINDOW + start, BLK), cols(h)]
            vt = vx[pl.ds(WINDOW + start, BLK), cols(h)]
            h1 = mm(wb[h, 0, 0], kt, NT) + mm(wb[h, 0, 1], kt, NT)
            h3 = mm(wb[h, 1, 0], kt, NT) + mm(wb[h, 1, 1], kt, NT)
            da = mm(wb[h, 2, 0], vt, NT) + mm(wb[h, 2, 1], vt, NT)
            r = rate[pl.ds(h, 1), pl.ds(start, BLK)]
            da = da * r
            sg = jax.nn.sigmoid(h1)
            sil = h1 * sg
            d1 = da * h3 * sg * (1.0 + h1 * (1.0 - sg))
            d3 = da * sil
            act = sil * h3 * r
            for n, value in enumerate((d1, d3, act)):
                hi, lo = split(value)
                dt[2 * n, :, pl.ds(start, BLK)] = hi
                dt[2 * n + 1, :, pl.ds(start, BLK)] = lo

        kh = kx[pl.ds(WINDOW, TOK), cols(h)]
        vh = vx[pl.ds(WINDOW, TOK), cols(h)]
        g[h, 0] = mm(dt[0], kh, NN) + mm(dt[1], kh, NN)
        g[h, 1] = mm(dt[2], kh, NN) + mm(dt[3], kh, NN)
        g[h, 2] = (mm(dt[4], vh, NN) + mm(dt[5], vh, NN)).T

    def remote(src, dst, send, recv, peer):
        return pltpu.make_async_remote_copy(
            src_ref=src, dst_ref=dst, send_sem=send, recv_sem=recv, device_id=peer, device_id_type=MESH
        )

    def start(copies):
        for copy in copies:
            copy.start()

    def halo(h):
        return [
            remote(
                ref.at[pl.ds(TOK, WINDOW), cols(h)],
                ref.at[pl.ds(0, WINDOW), cols(h)],
                halo_s.at[h, n],
                halo_r.at[h, n],
                {"seq": after},
            )
            for n, ref in enumerate((kx, vx))
        ]

    def reduce_x(h):
        return [
            remote(
                g.at[h, :, pl.ds(pl.multiple_of(((x + d) % XS) * 64, 64), 64), :],
                rx.at[h, d - 1],
                xs_s.at[h, d - 1],
                xs_r.at[h, d - 1],
                {"seq": x_peer(d)},
            )
            for d in range(1, XS)
        ]

    def reduce_z(h):
        return [
            remote(
                sx.at[h, :, pl.ds(pl.multiple_of(((zz + d) % ZS) * 8, 8), 8), :],
                rz.at[h, d - 1],
                zs_s.at[h, d - 1],
                zs_r.at[h, d - 1],
                {"seq": z_peer(d)},
            )
            for d in range(1, ZS)
        ]

    def gather_z(h):
        part = nt.at[h, :, pl.ds(pl.multiple_of(s * 8, 8), 8), :]
        return [
            remote(part, part, za_s.at[h, d - 1], za_r.at[h, d - 1], {"seq": z_peer(d)})
            for d in range(1, ZS)
        ]

    def gather_x(h):
        part = nt.at[h, :, pl.ds(pl.multiple_of(x * 64, 64), 64), :]
        return [
            remote(part, part, xa_s.at[h, d - 1], xa_r.at[h, d - 1], {"seq": x_peer(d)})
            for d in range(1, XS)
        ]

    def attend(h, b):
        begin = pl.multiple_of(b * BLK, BLK)
        span = BLK + WINDOW
        lanes = pl.ds(pl.multiple_of(h * FEAT, FEAT), FEAT)
        scores = mm(q[pl.ds(begin, BLK), lanes], kx[pl.ds(begin, span), lanes], NT) * (FEAT ** -0.5)
        rows = lax.broadcasted_iota(jnp.int32, (BLK, span), 0)
        keys = lax.broadcasted_iota(jnp.int32, (BLK, span), 1)
        first = jnp.where(s == 0, WINDOW - begin, 0)
        allowed = (keys > rows) & (keys <= rows + WINDOW) & (keys >= first)
        scores = jnp.where(allowed, scores, -jnp.inf)
        top = jnp.max(scores, axis=1, keepdims=True)
        expo = jnp.exp(scores - top)
        probs = (expo / jnp.sum(expo, axis=1, keepdims=True)).astype(BF16)
        out[pl.ds(begin, BLK), lanes] = mm(probs, vx[pl.ds(begin, span), lanes], NN)

    gradients(0)
    pl.semaphore_wait(barrier, greeted)
    halos = [halo(0), halo(1)]
    rxs = [reduce_x(0), reduce_x(1)]
    rzs = [reduce_z(0), reduce_z(1)]
    gzs = [gather_z(0), gather_z(1)]
    gxs = [gather_x(0), gather_x(1)]
    start(rxs[0])
    start(halos[0])
    gradients(1)
    start(rxs[1])

    @pl.loop(0, 4)
    def _(i):
        attend(i // 2, 2 + i % 2)

    def x_sum(h):
        for copy in rxs[h]:
            copy.wait_recv()
        own = g[h, :, pl.ds(pl.multiple_of(x * 64, 64), 64), :]
        sx[h] = own + rx[h, 0] + rx[h, 1] + rx[h, 2]
        start(rzs[h])

    x_sum(0)
    for copy in halos[0]:
        copy.wait_recv()

    @pl.loop(0, 2)
    def _(i):
        attend(0, i)

    x_sum(1)

    mine = pl.ds(pl.multiple_of(s * 8, 8), 8)

    def renorm(h):
        for copy in rzs[h]:
            copy.wait_recv()
        total = sx[h, :, pl.ds(pl.multiple_of(zz * 8, 8), 8), :]
        for d in range(ZS - 1):
            total = total + rz[h, d]
        weight = wt[h, :, mine, :]
        upd = weight + total
        old = jnp.sqrt(jnp.sum(weight * weight, axis=2, keepdims=True) + EPS)
        cur = jnp.sqrt(jnp.sum(upd * upd, axis=2, keepdims=True) + EPS)
        nt[h, :, mine, :] = upd * (old / cur)
        start(gzs[h])

    renorm(0)
    renorm(1)
    start(halos[1])
    for h in range(2):
        for copy in gzs[h]:
            copy.wait_recv()
        start(gxs[h])

    def final(h):
        for copy in gxs[h]:
            copy.wait_recv()
        for m in range(3):
            hi, lo = split(nt[h, m])
            nb[m, 0] = hi
            nb[m, 1] = lo

        @pl.loop(0, TOK // BLK)
        def _(i):
            begin = pl.multiple_of(i * BLK, BLK)
            qt = q[pl.ds(begin, BLK), cols(h)]
            p1 = mm(qt, nb[0, 0], NT) + mm(qt, nb[0, 1], NT)
            p3 = mm(qt, nb[1, 0], NT) + mm(qt, nb[1, 1], NT)
            hi, lo = split(p1 * jax.nn.sigmoid(p1) * p3)
            o = mm(hi, nb[2, 0], NT) + mm(lo, nb[2, 0], NT) + mm(hi, nb[2, 1], NT)
            z[pl.ds(begin, BLK), cols(h)] = o * hscale[h]

    final(0)
    final(1)

    lane = lax.broadcasted_iota(jnp.int32, (128, 128), 1)
    packed = jnp.zeros((128, 128), F32)
    for r in range(TOK // 128):
        zt = z[pl.ds(r * 128, 128), :]
        packed = jnp.where(lane == r, jnp.sum(zt * zt, axis=1, keepdims=True), packed)
    sq[0] = packed.T[:8, :]
    sqs = [
        remote(sq.at[0], sq.at[d], sq_s.at[d - 1], sq_r.at[d - 1], {"head": (me_h + d) % HS})
        for d in range(1, HS)
    ]
    start(sqs)

    news = []
    for h in range(2):
        for m, ref in enumerate((n1_hbm, n3_hbm, n2_hbm)):
            nout[h, m] = nt[h, m].T
            copy = pltpu.make_async_copy(nout.at[h, m], ref.at[h], out_sem.at[8 + 3 * h + m])
            copy.start()
            news.append(copy)

    for copy in halos[1]:
        copy.wait_recv()

    @pl.loop(0, 2)
    def _(i):
        attend(1, i)

    for copy in sqs:
        copy.wait_recv()
    total = sq[0]
    for d in range(1, HS):
        total = total + sq[d]
    inv = 1.0 / jnp.sqrt(total / (2 * HS * FEAT) + EPS)
    inv = jnp.concatenate([inv, jnp.zeros((120, 128), F32)], axis=0).T
    for r in range(TOK // 128):
        part = pl.ds(r * 128, 128)
        out[part, :] = out[part, :] + z[part, :] * inv[:, r : r + 1]
        copy = pltpu.make_async_copy(out.at[part, :], mixed_hbm.at[part, :], out_sem.at[r])
        copy.start()
        news.append(copy)
    for group in halos + rxs + rzs + gzs + gxs + [sqs]:
        for copy in group:
            copy.wait_send()
    for copy in news:
        copy.wait()


def per_device(queries, keys, values, rates, head_scale, w_one, w_three, w_two):
    any_space = pl.BlockSpec(memory_space=pl.ANY)
    dma = pltpu.SemaphoreType.DMA
    weight = jax.ShapeDtypeStruct((2, FEAT, FEAT), F32)
    return pl.pallas_call(
        layer,
        out_shape=(jax.ShapeDtypeStruct((TOK, 2 * FEAT), F32), weight, weight, weight),
        in_specs=[any_space] * 4 + [pl.BlockSpec(memory_space=pltpu.SMEM)] + [any_space] * 3,
        out_specs=(any_space,) * 4,
        scratch_shapes=[
            pltpu.VMEM((TOK, 2 * FEAT), BF16),
            pltpu.VMEM((TOK + WINDOW, 2 * FEAT), BF16),
            pltpu.VMEM((TOK + WINDOW, 2 * FEAT), BF16),
            pltpu.VMEM((2, TOK), F32),
            pltpu.VMEM((3, 2, FEAT, FEAT), F32),
            pltpu.VMEM((2, 3, FEAT, FEAT), F32),
            pltpu.VMEM((2, 3, 2, FEAT, FEAT), BF16),
            pltpu.VMEM((6, FEAT, TOK), BF16),
            pltpu.VMEM((2, 3, FEAT, FEAT), F32),
            pltpu.VMEM((2, XS - 1, 3, 64, FEAT), F32),
            pltpu.VMEM((2, 3, 64, FEAT), F32),
            pltpu.VMEM((2, ZS - 1, 3, 8, FEAT), F32),
            pltpu.VMEM((2, 3, FEAT, FEAT), F32),
            pltpu.VMEM((3, 2, FEAT, FEAT), BF16),
            pltpu.VMEM((2, 3, FEAT, FEAT), F32),
            pltpu.VMEM((TOK, 2 * FEAT), F32),
            pltpu.VMEM((TOK, 2 * FEAT), F32),
            pltpu.VMEM((HS, 8, 128), F32),
            dma((7,)),
            dma((14,)),
            dma((2, 2)),
            dma((2, 2)),
            dma((2, XS - 1)),
            dma((2, XS - 1)),
            dma((2, ZS - 1)),
            dma((2, ZS - 1)),
            dma((2, ZS - 1)),
            dma((2, ZS - 1)),
            dma((2, XS - 1)),
            dma((2, XS - 1)),
            dma((HS - 1,)),
            dma((HS - 1,)),
        ],
        compiler_params=pltpu.CompilerParams(
            collective_id=0, has_side_effects=True, vmem_limit_bytes=60 * 1024 * 1024
        ),
        name="layer",
    )(queries, keys, values, rates.T, head_scale, w_one, w_three, w_two)


def solution(mesh):
    tile = P("seq", "head")
    weight = P("head", None, None)
    return jax.shard_map(
        per_device,
        mesh=mesh,
        in_specs=(tile, tile, tile, tile, P("head"), weight, weight, weight),
        out_specs=(tile, weight, weight, weight),
        check_vma=False,
    )
```

```python
import jax
import jax.numpy as jnp
from jax import lax
from jax.experimental import pallas as pl
from jax.experimental.pallas import tpu as pltpu
from jax.sharding import PartitionSpec as P

WINDOW = 512
EPS = 1e-06
F32 = jnp.float32
BF16 = jnp.bfloat16
MESH = pl.DeviceIdType.MESH
scope = jax.named_scope
XS, ZS, HS = 4, 8, 8
TOK, FEAT, BLK = 1024, 256, 256
NT = (((1,), (1,)), ((), ()))
NN = (((1,), (0,)), ((), ()))


def mm(a, b, dims):
    return lax.dot_general(a, b, dims, preferred_element_type=F32)


def split(x):
    hi = x.astype(BF16)
    return hi, (x - hi.astype(F32)).astype(BF16)


def cols(h):
    return pl.ds(h * FEAT, FEAT)


LEVELS, BOTTOM = 250.0, 125.0
TINY = 1e-30


def encode(x, rate):
    code = jnp.exp2(jnp.abs(x) * rate - BOTTOM)
    return jnp.where(x < 0, -code, code)


def decode(code, step):
    code = code.astype(F32)
    value = (jnp.log2(jnp.abs(code)) + BOTTOM) * step
    return jnp.where(code < 0, -value, value)


def scale_of(x, axis):
    top = jnp.max(jnp.abs(x), axis=axis, keepdims=True) * (1.0 + 2.0 ** -6) + TINY
    return top.astype(BF16).astype(F32)


def pick_rows(rows, shape, axis):
    index = lax.broadcasted_iota(jnp.int32, shape, axis)
    return jnp.where(index == 0, rows[0], jnp.where(index == 1, rows[1], rows[2]))


def encode_root(x, old):
    code = jnp.exp2(jnp.sqrt(jnp.minimum(jnp.abs(x) / old, 1.0)) * LEVELS - BOTTOM)
    return jnp.where(x < 0, -code, code)


def decode_root(code, old):
    code = code.astype(F32)
    root = (jnp.log2(jnp.abs(code)) + BOTTOM) * (1.0 / LEVELS)
    value = root * root * old
    return jnp.where(code < 0, -value, value)


def layer(
    q_hbm, k_hbm, v_hbm, rate_hbm, hscale_hbm, w1_hbm, w3_hbm, w2_hbm,
    out, z, inv_out, nout,
    q, kx, vx, rate, hscale, w, wt, wb, old, dt, g, gc, rx, sx, sc, rz, nc, nb, sq, relay,
    in_sem, halo_s, halo_r, leg_s, leg_r, xs_s, xs_r, zs_s, zs_r, za_s, za_r, xa_s, xa_r, sq_s, sq_r,
):
    s = lax.axis_index("seq")
    me_h = lax.axis_index("head")
    x = s // ZS
    zz = s % ZS

    def x_peer(d):
        return ((x + d) % XS) * ZS + zz

    def z_peer(d):
        return x * ZS + (zz + d) % ZS

    barrier = pltpu.get_barrier_semaphore()
    greeted = 0
    for d in range(1, XS):
        pl.semaphore_signal(barrier, inc=1, device_id={"seq": x_peer(d)}, device_id_type=MESH)
        greeted += 1
    for d in range(1, ZS):
        pl.semaphore_signal(barrier, inc=1, device_id={"seq": z_peer(d)}, device_id_type=MESH)
        greeted += 1
    for d in range(1, HS):
        pl.semaphore_signal(barrier, inc=1, device_id={"head": (me_h + d) % HS}, device_id_type=MESH)
        greeted += 1
    after = (s + 1) % (XS * ZS)
    for peer in (after, (s + XS * ZS - 1) % (XS * ZS)):
        pl.semaphore_signal(barrier, inc=1, device_id={"seq": peer}, device_id_type=MESH)
        greeted += 1

    def fetch(src, dst, i):
        copy = pltpu.make_async_copy(src, dst, in_sem.at[i])
        copy.start()
        return copy

    loads = [
        fetch(w1_hbm, w.at[0], 0),
        fetch(w3_hbm, w.at[1], 1),
        fetch(w2_hbm, w.at[2], 2),
        fetch(k_hbm, kx.at[pl.ds(WINDOW, TOK), :], 3),
        fetch(v_hbm, vx.at[pl.ds(WINDOW, TOK), :], 4),
        fetch(rate_hbm, rate, 5),
        fetch(q_hbm, q, 6),
        fetch(hscale_hbm, hscale, 7),
    ]

    @pl.when(s == 0)
    def _():
        kx[pl.ds(0, WINDOW), :] = jnp.zeros((WINDOW, 2 * FEAT), BF16)
        vx[pl.ds(0, WINDOW), :] = jnp.zeros((WINDOW, 2 * FEAT), BF16)

    with scope("load_w"):
        for load in loads[:3]:
            load.wait()
    for h in range(2):
        for m in range(3):
            turned = w[m, h].T
            wt[h, m] = turned
            old[h, m] = jnp.sqrt(jnp.sum(turned * turned, axis=1, keepdims=True) + EPS)
        for m in range(2):
            hi, lo = split(wt[h, m])
            wb[h, m, 0] = hi
            wb[h, m, 1] = lo
        hi, lo = split(w[2, h])
        wb[h, 2, 0] = hi
        wb[h, 2, 1] = lo
    with scope("load_x"):
        for load in loads[3:6]:
            load.wait()

    def gradients(h):
        @pl.loop(0, TOK // BLK)
        def _(i):
            start = pl.multiple_of(i * BLK, BLK)
            kt = kx[pl.ds(WINDOW + start, BLK), cols(h)]
            vt = vx[pl.ds(WINDOW + start, BLK), cols(h)]
            h1 = mm(wb[h, 0, 0], kt, NT) + mm(wb[h, 0, 1], kt, NT)
            h3 = mm(wb[h, 1, 0], kt, NT) + mm(wb[h, 1, 1], kt, NT)
            da = mm(wb[h, 2, 0], vt, NT) + mm(wb[h, 2, 1], vt, NT)
            r = rate[pl.ds(h, 1), pl.ds(start, BLK)]
            da = da * r
            sg = jax.nn.sigmoid(h1)
            sil = h1 * sg
            d1 = da * h3 * sg * (1.0 + h1 * (1.0 - sg))
            d3 = da * sil
            act = sil * h3 * r
            for n, value in enumerate((d1, d3, act)):
                hi, lo = split(value)
                dt[2 * n, :, pl.ds(start, BLK)] = hi
                dt[2 * n + 1, :, pl.ds(start, BLK)] = lo

        kh = kx[pl.ds(WINDOW, TOK), cols(h)]
        vh = vx[pl.ds(WINDOW, TOK), cols(h)]
        g[h, 0] = mm(dt[0], kh, NN) + mm(dt[1], kh, NN)
        g[h, 1] = mm(dt[2], kh, NN) + mm(dt[3], kh, NN)
        g[h, 2] = (mm(dt[4], vh, NN) + mm(dt[5], vh, NN)).T
        scales = []
        for m in range(3):
            value = g[h, m].reshape(XS, 64, FEAT)
            scale = scale_of(value, 1)
            scales.append(scale)
            gc[h, :, pl.ds(64 * m, 64), :] = encode(value, LEVELS / scale).astype(BF16)
        gc[h, :, pl.ds(192, 8), :] = pick_rows(scales, (XS, 8, FEAT), 1).astype(BF16)

    def remote(src, dst, send, recv, peer):
        return pltpu.make_async_remote_copy(
            src_ref=src, dst_ref=dst, send_sem=send, recv_sem=recv, device_id=peer, device_id_type=MESH
        )

    def start(copies):
        for copy in copies:
            copy.start()

    def halo(h):
        return [
            remote(
                ref.at[pl.ds(TOK, WINDOW), cols(h)],
                ref.at[pl.ds(0, WINDOW), cols(h)],
                halo_s.at[h, n],
                halo_r.at[h, n],
                {"seq": after},
            )
            for n, ref in enumerate((kx, vx))
        ]

    def relay_in(h):
        return remote(
            vx.at[pl.ds(TOK, WINDOW), cols(h)], relay.at[h], leg_s.at[h], leg_r.at[h], {"seq": x_peer(1)}
        )

    def relay_out(h):
        return remote(
            relay.at[h], vx.at[pl.ds(0, WINDOW), cols(h)], halo_s.at[h, 2], halo_r.at[h, 1], {"seq": z_peer(1)}
        )

    not_last = s < XS * ZS - 1
    inner = zz < ZS - 1
    leaves = (zz == ZS - 1) & (x < XS - 1)
    relays = (zz == ZS - 1) & (x > 0)

    def send_halo(h):
        ks, vs = halo(h)

        @pl.when(not_last)
        def _():
            ks.start()

        @pl.when(inner)
        def _():
            vs.start()

    def send_leg(h):
        @pl.when(leaves)
        def _():
            relay_in(h).start()

    def send_relay(h):
        @pl.when(relays)
        def _():
            relay_in(h).wait_recv()
            relay_out(h).start()

    def await_halo(h):
        ks, vs = halo(h)

        @pl.when(s > 0)
        def _():
            ks.wait_recv()
            vs.wait_recv()

    def drain_halo(h):
        ks, vs = halo(h)

        @pl.when(not_last)
        def _():
            ks.wait_send()

        @pl.when(inner)
        def _():
            vs.wait_send()

        @pl.when(leaves)
        def _():
            relay_in(h).wait_send()

        @pl.when(relays)
        def _():
            relay_out(h).wait_send()

    def reduce_x(h):
        return [
            remote(
                gc.at[h, (x + d) % XS], rx.at[h, d - 1], xs_s.at[h, d - 1], xs_r.at[h, d - 1], {"seq": x_peer(d)}
            )
            for d in range(1, XS)
        ]

    def reduce_z(h):
        return [
            remote(
                sc.at[h, (zz + d) % ZS], rz.at[h, d - 1], zs_s.at[h, d - 1], zs_r.at[h, d - 1], {"seq": z_peer(d)}
            )
            for d in range(1, ZS)
        ]

    def gather_z(h):
        part = nc.at[h, x, zz]
        return [
            remote(part, part, za_s.at[h, d - 1], za_r.at[h, d - 1], {"seq": z_peer(d)})
            for d in range(1, ZS)
        ]

    def gather_x(h):
        part = nc.at[h, x]
        return [
            remote(part, part, xa_s.at[h, d - 1], xa_r.at[h, d - 1], {"seq": x_peer(d)})
            for d in range(1, XS)
        ]

    def attend(h, b):
        begin = pl.multiple_of(b * BLK, BLK)
        span = BLK + WINDOW
        lanes = pl.ds(pl.multiple_of(h * FEAT, FEAT), FEAT)
        scores = mm(q[pl.ds(begin, BLK), lanes], kx[pl.ds(begin, span), lanes], NT) * (FEAT ** -0.5)
        rows = lax.broadcasted_iota(jnp.int32, (BLK, span), 0)
        keys = lax.broadcasted_iota(jnp.int32, (BLK, span), 1)
        first = jnp.where(s == 0, WINDOW - begin, 0)
        allowed = (keys > rows) & (keys <= rows + WINDOW) & (keys >= first)
        scores = jnp.where(allowed, scores, -jnp.inf)
        top = jnp.max(scores, axis=1, keepdims=True)
        expo = jnp.exp(scores - top)
        probs = (expo / jnp.sum(expo, axis=1, keepdims=True)).astype(BF16)
        out[pl.ds(begin, BLK), lanes] = mm(probs, vx[pl.ds(begin, span), lanes], NN)

    with scope("greet"):
        pl.semaphore_wait(barrier, greeted)
    rxs = [reduce_x(0), reduce_x(1)]
    rzs = [reduce_z(0), reduce_z(1)]
    gzs = [gather_z(0), gather_z(1)]
    gxs = [gather_x(0), gather_x(1)]
    send_leg(0)
    send_halo(0)
    with scope("grad0"):
        gradients(0)
    start(rxs[0])
    with scope("grad1"):
        gradients(1)
    start(rxs[1])
    with scope("relay0"):
        send_relay(0)
    loads[6].wait()
    loads[7].wait()

    with scope("attn_local"):

        @pl.loop(0, 4)
        def _(i):
            attend(i // 2, 2 + i % 2)

    def x_sum(h):
        with scope(f"wait_rx{h}"):
            for copy in rxs[h]:
                copy.wait_recv()
        steps = [rx[h, d, pl.ds(192, 8), :].astype(F32) * (1.0 / LEVELS) for d in range(XS - 1)]
        codes, scales = [], []
        for m in range(3):
            total = g[h, m, pl.ds(pl.multiple_of(x * 64, 64), 64), :]
            for d in range(XS - 1):
                total = total + decode(rx[h, d, pl.ds(64 * m, 64), :], steps[d][m : m + 1, :])
            sx[h, m] = total
            scale = scale_of(total, 0)
            scales.append(scale)
            codes.append(encode(total, LEVELS / scale).reshape(ZS, 8, FEAT))
        codes.append(jnp.broadcast_to(pick_rows(scales, (8, FEAT), 0), (ZS, 8, FEAT)))
        sc[h] = jnp.concatenate(codes, axis=1).astype(BF16)
        start(rzs[h])

    x_sum(0)
    send_leg(1)
    with scope("wait_halo0"):
        await_halo(0)

    with scope("attn_h0"):

        @pl.loop(0, 2)
        def _(i):
            attend(0, i)

    x_sum(1)

    mine = pl.ds(pl.multiple_of(s * 8, 8), 8)

    def renorm(h):
        with scope(f"wait_rz{h}"):
            for copy in rzs[h]:
                copy.wait_recv()
        codes = [rz[h, d].astype(F32) for d in range(ZS - 1)]
        parts = []
        for m in range(3):
            total = sx[h, m, pl.ds(pl.multiple_of(zz * 8, 8), 8), :]
            for code in codes:
                total = total + decode(code[8 * m : 8 * m + 8, :], code[24 + m : 25 + m, :] * (1.0 / LEVELS))
            upd = wt[h, m, mine, :] + total
            was = old[h, m, mine, :]
            cur = jnp.sqrt(jnp.sum(upd * upd, axis=1, keepdims=True) + EPS)
            parts.append(encode_root(upd * (was / cur), was))
        nc[h, x, zz] = jnp.concatenate(parts, axis=0).astype(BF16)
        start(gzs[h])

    renorm(0)
    renorm(1)
    send_halo(1)
    with scope("relay1"):
        send_relay(1)
    for h in range(2):
        with scope(f"wait_gz{h}"):
            for copy in gzs[h]:
                copy.wait_recv()
        start(gxs[h])

    def final(h):
        with scope(f"wait_gx{h}"):
            for copy in gxs[h]:
                copy.wait_recv()
        for m in range(3):
            fresh = decode_root(nc[h, :, :, pl.ds(8 * m, 8), :].reshape(FEAT, FEAT), old[h, m])
            hi, lo = split(fresh)
            nb[m, 0] = hi
            nb[m, 1] = lo
            g[h, m] = fresh

        @pl.loop(0, TOK // BLK)
        def _(i):
            begin = pl.multiple_of(i * BLK, BLK)
            qt = q[pl.ds(begin, BLK), cols(h)]
            p1 = mm(qt, nb[0, 0], NT) + mm(qt, nb[0, 1], NT)
            p3 = mm(qt, nb[1, 0], NT) + mm(qt, nb[1, 1], NT)
            hi, lo = split(p1 * jax.nn.sigmoid(p1) * p3)
            o = mm(hi, nb[2, 0], NT) + mm(lo, nb[2, 0], NT) + mm(hi, nb[2, 1], NT)
            z[pl.ds(begin, BLK), cols(h)] = o * hscale[h]

    with scope("final0"):
        final(0)
    with scope("final1"):
        final(1)

    lane = lax.broadcasted_iota(jnp.int32, (128, 128), 1)
    packed = jnp.zeros((128, 128), F32)
    for r in range(TOK // 128):
        zt = z[pl.ds(r * 128, 128), :]
        packed = jnp.where(lane == r, jnp.sum(zt * zt, axis=1, keepdims=True), packed)
    sq[0] = packed.T[:8, :]
    sqs = [
        remote(sq.at[0], sq.at[d], sq_s.at[d - 1], sq_r.at[d - 1], {"head": (me_h + d) % HS})
        for d in range(1, HS)
    ]
    start(sqs)

    for h in range(2):
        for m in range(3):
            nout[m, h] = g[h, m].T

    with scope("wait_halo1"):
        await_halo(1)

    with scope("attn_h1"):

        @pl.loop(0, 2)
        def _(i):
            attend(1, i)

    with scope("wait_sq"):
        for copy in sqs:
            copy.wait_recv()
    total = sq[0]
    for d in range(1, HS):
        total = total + sq[d]
    inv = 1.0 / jnp.sqrt(total / (2 * HS * FEAT) + EPS)
    inv_out[...] = jnp.concatenate([inv, jnp.zeros((120, 128), F32)], axis=0).T
    with scope("wait_end"):
        for group in rxs + rzs + gzs + gxs + [sqs]:
            for copy in group:
                copy.wait_send()
        drain_halo(0)
        drain_halo(1)


def combine(attn, z, inv, fresh, mixed_hbm, n1_hbm, n3_hbm, n2_hbm, out, sem):
    copies = [
        pltpu.make_async_copy(fresh.at[m], ref, sem.at[8 + m])
        for m, ref in enumerate((n1_hbm, n3_hbm, n2_hbm))
    ]
    for copy in copies:
        copy.start()
    scale = inv[...]
    for r in range(TOK // 128):
        part = pl.ds(r * 128, 128)
        out[part, :] = attn[part, :] + z[part, :] * scale[:, r : r + 1]
        copy = pltpu.make_async_copy(out.at[part, :], mixed_hbm.at[part, :], sem.at[r])
        copy.start()
        copies.append(copy)
    for copy in copies:
        copy.wait()


def per_device(queries, keys, values, rates, head_scale, w_one, w_three, w_two):
    any_space = pl.BlockSpec(memory_space=pltpu.HBM)
    vmem = pl.BlockSpec(memory_space=pltpu.VMEM)
    dma = pltpu.SemaphoreType.DMA
    rows = jax.ShapeDtypeStruct((TOK, 2 * FEAT), F32)
    weight = jax.ShapeDtypeStruct((2, FEAT, FEAT), F32)
    pinned = [
        pltpu.with_memory_space_constraint(a, pltpu.HBM) for a in (queries, keys, values, rates.T, head_scale, w_one, w_three, w_two)
    ]
    attn, z, inv, fresh = pl.pallas_call(
        layer,
        out_shape=(rows, rows, jax.ShapeDtypeStruct((128, 128), F32), jax.ShapeDtypeStruct((3, 2, FEAT, FEAT), F32)),
        in_specs=[any_space] * 8,
        out_specs=(vmem,) * 4,
        scratch_shapes=[
            pltpu.VMEM((TOK, 2 * FEAT), BF16),
            pltpu.VMEM((TOK + WINDOW, 2 * FEAT), BF16),
            pltpu.VMEM((TOK + WINDOW, 2 * FEAT), BF16),
            pltpu.VMEM((2, TOK), F32),
            pltpu.SMEM((2,), F32),
            pltpu.VMEM((3, 2, FEAT, FEAT), F32),
            pltpu.VMEM((2, 3, FEAT, FEAT), F32),
            pltpu.VMEM((2, 3, 2, FEAT, FEAT), BF16),
            pltpu.VMEM((2, 3, FEAT, 1), F32),
            pltpu.VMEM((6, FEAT, TOK), BF16),
            pltpu.VMEM((2, 3, FEAT, FEAT), F32),
            pltpu.VMEM((2, XS, 200, FEAT), BF16),
            pltpu.VMEM((2, XS - 1, 200, FEAT), BF16),
            pltpu.VMEM((2, 3, 64, FEAT), F32),
            pltpu.VMEM((2, ZS, 32, FEAT), BF16),
            pltpu.VMEM((2, ZS - 1, 32, FEAT), BF16),
            pltpu.VMEM((2, XS, ZS, 24, FEAT), BF16),
            pltpu.VMEM((3, 2, FEAT, FEAT), BF16),
            pltpu.VMEM((HS, 8, 128), F32),
            pltpu.VMEM((2, WINDOW, FEAT), BF16),
            dma((8,)),
            dma((2, 3)),
            dma((2, 2)),
            dma((2,)),
            dma((2,)),
            dma((2, XS - 1)),
            dma((2, XS - 1)),
            dma((2, ZS - 1)),
            dma((2, ZS - 1)),
            dma((2, ZS - 1)),
            dma((2, ZS - 1)),
            dma((2, XS - 1)),
            dma((2, XS - 1)),
            dma((HS - 1,)),
            dma((HS - 1,)),
        ],
        compiler_params=pltpu.CompilerParams(
            collective_id=0, has_side_effects=True, vmem_limit_bytes=40 * 1024 * 1024
        ),
        name="layer",
    )(*pinned)
    return pl.pallas_call(
        combine,
        out_shape=(rows, weight, weight, weight),
        in_specs=[vmem] * 4,
        out_specs=(any_space,) * 4,
        scratch_shapes=[pltpu.VMEM((TOK, 2 * FEAT), F32), dma((11,))],
        compiler_params=pltpu.CompilerParams(vmem_limit_bytes=16 * 1024 * 1024),
        name="combine",
    )(attn, z, inv, fresh)


def solution(mesh):
    tile = P("seq", "head")
    weight = P("head", None, None)
    return jax.shard_map(
        per_device,
        mesh=mesh,
        in_specs=(tile, tile, tile, tile, P("head"), weight, weight, weight),
        out_specs=(tile, weight, weight, weight),
        check_vma=False,
    )
```

```python
import math
import jax
import jax.numpy as jnp
from jax import lax
from jax.experimental import pallas as pl
from jax.experimental.pallas import tpu as pltpu
from jax.sharding import PartitionSpec as P

WINDOW = 512
EPS = 1e-06
F32 = jnp.float32
BF16 = jnp.bfloat16
MESH = pl.DeviceIdType.MESH
scope = jax.named_scope
XS, ZS, HS = 4, 8, 8
TOK, FEAT, BLK = 1024, 256, 256
NT = (((1,), (1,)), ((), ()))
NN = (((1,), (0,)), ((), ()))


def mm(a, b, dims):
    return lax.dot_general(a, b, dims, preferred_element_type=F32)


def split(x):
    hi = x.astype(BF16)
    return hi, (x - hi.astype(F32)).astype(BF16)


def cols(h):
    return pl.ds(h * FEAT, FEAT)


LEVELS, BOTTOM = 250.0, 125.0
SOFT = math.log2(math.e) * FEAT ** -0.5
GROUPS = ((0, (0, 1)), (0, (2,)), (1, (0, 1)), (1, (2,)))
TINY = 1e-30


def sigmoid(x):
    return 0.5 * jnp.tanh(0.5 * x) + 0.5


def encode(x, rate):
    code = jnp.exp2(jnp.abs(x) * rate - BOTTOM)
    return jnp.where(x < 0, -code, code)


def decode(code, step):
    code = code.astype(F32)
    value = (jnp.log2(jnp.abs(code)) + BOTTOM) * step
    return jnp.where(code < 0, -value, value)


def scale_of(x, axis):
    top = jnp.max(jnp.abs(x), axis=axis, keepdims=True) * (1.0 + 2.0 ** -6) + TINY
    return top.astype(BF16).astype(F32)


def pick_rows(rows, shape, axis):
    if len(rows) == 1:
        return jnp.broadcast_to(rows[0], shape)
    index = lax.broadcasted_iota(jnp.int32, shape, axis)
    return jnp.where(index == 0, rows[0], rows[1])


def encode_root(x, old):
    code = jnp.exp2(jnp.sqrt(jnp.minimum(jnp.abs(x) / old, 1.0)) * LEVELS - BOTTOM)
    return jnp.where(x < 0, -code, code)


def decode_root(code, old):
    code = code.astype(F32)
    root = (jnp.log2(jnp.abs(code)) + BOTTOM) * (1.0 / LEVELS)
    value = root * root * old
    return jnp.where(code < 0, -value, value)


def layer(
    q_hbm, k_hbm, v_hbm, rate_hbm, hscale_hbm, w1_hbm, w3_hbm, w2_hbm,
    out, z, inv_out, nout,
    q, kx, vx, rate, hscale, w, wt, wb, old, dt, g, gc, rx, sx, sc, rz, nc, nb, act, sq, kh, vh, v_relay, qh, qh0, q_relay, st, st_in, st_joint, st_back, oc, oc0, oh, oh0, o_relay,
    in_sem, hs, hr, xs_s, xs_r, zs_s, zs_r, za_s, za_r, xa_s, xa_r, sq_s, sq_r,
):
    s = lax.axis_index("seq")
    me_h = lax.axis_index("head")
    x = s // ZS
    zz = s % ZS

    def x_peer(d):
        return ((x + d) % XS) * ZS + zz

    def z_peer(d):
        return x * ZS + (zz + d) % ZS

    barrier = pltpu.get_barrier_semaphore()
    greeted = 0
    for d in range(1, XS):
        pl.semaphore_signal(barrier, inc=1, device_id={"seq": x_peer(d)}, device_id_type=MESH)
        greeted += 1
    for d in range(1, ZS):
        pl.semaphore_signal(barrier, inc=1, device_id={"seq": z_peer(d)}, device_id_type=MESH)
        greeted += 1
    for d in range(1, HS):
        pl.semaphore_signal(barrier, inc=1, device_id={"head": (me_h + d) % HS}, device_id_type=MESH)
        greeted += 1
    after = (s + 1) % (XS * ZS)
    before = (s + XS * ZS - 1) % (XS * ZS)
    for peer in (after, before):
        pl.semaphore_signal(barrier, inc=1, device_id={"seq": peer}, device_id_type=MESH)
        greeted += 1

    def fetch(src, dst, i):
        copy = pltpu.make_async_copy(src, dst, in_sem.at[i])
        copy.start()
        return copy

    def fetch_head(h):
        return [
            fetch(w1_hbm.at[h], w.at[0, h], 8 * h),
            fetch(w3_hbm.at[h], w.at[1, h], 8 * h + 1),
            fetch(w2_hbm.at[h], w.at[2, h], 8 * h + 2),
            fetch(k_hbm.at[:, cols(h)], kx.at[:, cols(h)], 8 * h + 3),
            fetch(v_hbm.at[:, cols(h)], vx.at[:, cols(h)], 8 * h + 4),
        ]

    loads = [fetch_head(0)]
    rate_load = fetch(rate_hbm, rate, 5)
    front = pl.ds(0, WINDOW)
    back = pl.ds(WINDOW, WINDOW)
    q_load = fetch(q_hbm.at[front, :], q.at[front, :], 6)
    loads.append(fetch_head(1))
    late_loads = [fetch(q_hbm.at[back, :], q.at[back, :], 13), fetch(hscale_hbm, hscale, 7)]

    def prepare(h):
        with scope(f"load{h}"):
            for load in loads[h][:3] if h == 0 else loads[h]:
                load.wait()
        for m in range(3):
            turned = w[m, h].T
            wt[h, m] = turned
            old[h, m] = jnp.sqrt(jnp.sum(turned * turned, axis=1, keepdims=True) + EPS)
        for m in range(2):
            hi, lo = split(wt[h, m])
            wb[h, m, 0] = hi
            wb[h, m, 1] = lo
        hi, lo = split(w[2, h])
        wb[h, 2, 0] = hi
        wb[h, 2, 1] = lo

    def gradients(h):
        @pl.loop(0, TOK // BLK, unroll=True)
        def _(i):
            start = pl.multiple_of(i * BLK, BLK)
            kt = kx[pl.ds(start, BLK), cols(h)]
            vt = vx[pl.ds(start, BLK), cols(h)]
            h1 = mm(wb[h, 0, 0], kt, NT) + mm(wb[h, 0, 1], kt, NT)
            h3 = mm(wb[h, 1, 0], kt, NT) + mm(wb[h, 1, 1], kt, NT)
            da = mm(wb[h, 2, 0], vt, NT) + mm(wb[h, 2, 1], vt, NT)
            r = rate[pl.ds(h, 1), pl.ds(start, BLK)]
            da = da * r
            sg = sigmoid(h1)
            sil = h1 * sg
            d1 = da * h3 * sg * (1.0 + h1 * (1.0 - sg))
            d3 = da * sil
            act = sil * h3 * r
            for n, value in enumerate((d1, d3, act)):
                hi, lo = split(value)
                dt[2 * n, :, pl.ds(start, BLK)] = hi
                dt[2 * n + 1, :, pl.ds(start, BLK)] = lo

        kh = kx[:, cols(h)]
        vh = vx[:, cols(h)]
        g[h, 0] = mm(dt[0], kh, NN) + mm(dt[1], kh, NN)
        g[h, 1] = mm(dt[2], kh, NN) + mm(dt[3], kh, NN)
        pack_share(2 * h)
        g[h, 2] = (mm(dt[4], vh, NN) + mm(dt[5], vh, NN)).T
        start(reduce_x(2 * h))
        pack_share(2 * h + 1)
        start(reduce_x(2 * h + 1))

    def pack_share(i):
        h, ms = GROUPS[i]
        scales = []
        for n, m in enumerate(ms):
            value = g[h, m].reshape(XS, 64, FEAT)
            scale = scale_of(value, 1)
            scales.append(scale)
            gc[i, :, pl.ds(64 * n, 64), :] = encode(value, LEVELS / scale).astype(BF16)
        gc[i, :, pl.ds(64 * len(ms), 8), :] = pick_rows(scales, (XS, 8, FEAT), 1).astype(BF16)

    def remote(src, dst, send, recv, peer):
        return pltpu.make_async_remote_copy(
            src_ref=src, dst_ref=dst, send_sem=send, recv_sem=recv, device_id=peer, device_id_type=MESH
        )

    def start(copies):
        for copy in copies:
            copy.start()

    last = XS * ZS - 1

    def block(n):
        return pl.ds(n * BLK, BLK)

    tail = pl.ds(TOK - BLK, BLK)

    def k_copy():
        return remote(kx.at[tail, cols(0)], kh, hs.at[0], hr.at[0], {"seq": after})

    def v_copy():
        return remote(vx.at[tail, cols(0)], vh, hs.at[1], hr.at[1], {"seq": after})

    def v_leg():
        return remote(vx.at[tail, cols(0)], v_relay, hs.at[2], hr.at[2], {"seq": x_peer(1)})

    def v_forward():
        return remote(v_relay, vh, hs.at[3], hr.at[1], {"seq": z_peer(1)})

    def query_copy():
        return remote(q.at[front, cols(1)], qh, hs.at[4], hr.at[3], {"seq": before})

    def query_leg():
        return remote(q.at[front, cols(1)], q_relay, hs.at[5], hr.at[4], {"seq": x_peer(XS - 1)})

    def query_forward():
        return remote(q_relay, qh, hs.at[6], hr.at[3], {"seq": z_peer(ZS - 1)})

    def stat_copy():
        return remote(st, st_in, hs.at[7], hr.at[5], {"seq": before})

    def attn_copy():
        return remote(oc, oh, hs.at[8], hr.at[6], {"seq": after})

    def attn_leg():
        return remote(oc, o_relay, hs.at[9], hr.at[7], {"seq": x_peer(1)})

    def attn_forward():
        return remote(o_relay, oh, hs.at[10], hr.at[6], {"seq": z_peer(1)})

    def total_copy():
        return remote(st_joint, st_back, hs.at[11], hr.at[8], {"seq": after})

    def query0_copy():
        return remote(q.at[block(0), cols(0)], qh0, hs.at[12], hr.at[9], {"seq": before})

    def attn0_copy():
        return remote(oc0, oh0, hs.at[13], hr.at[10], {"seq": after})

    low, high = zz == 0, zz == ZS - 1
    transfers = {
        "k": (s < last, k_copy),
        "v": (zz < ZS - 1, v_copy),
        "v_leg": (high & (x < XS - 1), v_leg),
        "v_forward": (high & (x > 0), v_forward),
        "query": (zz > 0, query_copy),
        "query_leg": (low & (x > 0), query_leg),
        "query_forward": (low & (x < XS - 1), query_forward),
        "stat": (s > 0, stat_copy),
        "attn": (zz < ZS - 1, attn_copy),
        "attn_leg": (high & (x < XS - 1), attn_leg),
        "attn_forward": (high & (x > 0), attn_forward),
        "total": (s < last, total_copy),
        "query0": (s > 0, query0_copy),
        "attn0": (s < last, attn0_copy),
    }

    def send(*names):
        for name in names:
            wanted, copy = transfers[name]

            @pl.when(wanted)
            def _():
                copy().start()

    def pass_on(leg, forward):
        @pl.when(transfers[forward][0])
        def _():
            leg().wait_recv()
            transfers[forward][1]().start()

    def drain_halo():
        for wanted, copy in transfers.values():

            @pl.when(wanted)
            def _():
                copy().wait_send()

    def reduce_x(i):
        rows = pl.ds(0, 64 * len(GROUPS[i][1]) + 8)
        return [
            remote(
                gc.at[i, (x + d) % XS, rows, :],
                rx.at[i, d - 1, rows, :],
                xs_s.at[i, d - 1],
                xs_r.at[i, d - 1],
                {"seq": x_peer(d)},
            )
            for d in range(1, XS)
        ]

    def reduce_z(i):
        rows = pl.ds(0, 8 * len(GROUPS[i][1]) + 8)
        return [
            remote(
                sc.at[i, (zz + d) % ZS, rows, :],
                rz.at[i, d - 1, rows, :],
                zs_s.at[i, d - 1],
                zs_r.at[i, d - 1],
                {"seq": z_peer(d)},
            )
            for d in range(1, ZS)
        ]

    def gather_z(i):
        part = nc.at[i, x, zz, pl.ds(0, 8 * len(GROUPS[i][1])), :]
        return [
            remote(part, part, za_s.at[i, d - 1], za_r.at[i, d - 1], {"seq": z_peer(d)})
            for d in range(1, ZS)
        ]

    def gather_x(i):
        part = nc.at[i, x, :, pl.ds(0, 8 * len(GROUPS[i][1])), :]
        return [
            remote(part, part, xa_s.at[i, d - 1], xa_r.at[i, d - 1], {"seq": x_peer(d)})
            for d in range(1, XS)
        ]

    def received(copies):
        for copy in copies:
            copy.wait_recv()

    tile_rows = lax.broadcasted_iota(jnp.int32, (BLK, BLK), 0)
    tile_keys = lax.broadcasted_iota(jnp.int32, (BLK, BLK), 1)

    def older(scores):
        return jnp.where(tile_keys > tile_rows, scores, -jnp.inf)

    def newer(scores):
        return jnp.where(tile_keys <= tile_rows, scores, -jnp.inf)

    def row_max(tiles):
        top = tiles[0]
        for tile in tiles[1:]:
            top = jnp.maximum(top, tile)
        return jnp.max(top, axis=1, keepdims=True)

    def row_sum(tiles):
        total = tiles[0]
        for tile in tiles[1:]:
            total = total + tile
        return jnp.sum(total, axis=1, keepdims=True)

    def expos(tiles, top):
        return [jnp.exp2((tile - top) * SOFT) for tile in tiles]

    def weigh(tiles, total, values):
        scale = 1.0 / total
        result = None
        for tile, value in zip(tiles, values):
            part = mm((tile * scale).astype(BF16), value, NN)
            result = part if result is None else result + part
        return result

    def attend(h, b):
        qt = q[block(b), cols(h)]
        tiles, values = [], []
        for i, n in enumerate((b - 2, b - 1, b)):
            tile = mm(qt, kx[block(n), cols(h)] if n >= 0 else kh[...], NT)
            if i == 0:
                tile = older(tile)
            if i == 2:
                tile = newer(tile)
            if n < 0:
                tile = jnp.where(s == 0, -jnp.inf, tile)
            tiles.append(tile)
            values.append(vx[block(n), cols(h)] if n >= 0 else vh[...])
        tiles = expos(tiles, row_max(tiles))
        out[block(b), cols(h)] = weigh(tiles, row_sum(tiles), values)

    lane = lax.broadcasted_iota(jnp.int32, (128, 128), 1)

    def to_rows(columns):
        packed = jnp.zeros((128, 128), F32)
        for n, column in enumerate(columns):
            packed = jnp.where(lane == n, column, packed)
        return packed.T

    def to_columns(rows):
        turned = jnp.concatenate([rows, jnp.zeros((112, 128), F32)], axis=0).T
        return [
            jnp.concatenate([turned[:, 2 * b : 2 * b + 1], turned[:, 2 * b + 1 : 2 * b + 2]], axis=0)
            for b in range(6)
        ]

    def halves(column):
        return [column[:128], column[128:]]

    shared = ((1, 0), (1, 1), (0, 0))

    def near_tiles(h, b):
        qt = q[block(b), cols(h)]
        tiles = [mm(qt, kx[block(n), cols(h)], NT) for n in range(b + 1)]
        tiles[b] = newer(tiles[b])
        values = [vx[block(n), cols(h)] for n in range(b + 1)]
        if h == 0:
            tiles.append(jnp.where(s == 0, -jnp.inf, mm(qt, kh[...], NT)))
            values.append(vh[...])
        return tiles, values

    def near_stats():
        tops, sums = [], []
        for h, b in shared:
            tiles, _ = near_tiles(h, b)
            top = row_max(tiles)
            tops += halves(top)
            sums += halves(row_sum(expos(tiles, top)))
        st[...] = to_rows(tops + sums)[:16]

    def await_query():
        @pl.when(s < last)
        def _():
            query0_copy().wait_recv()
            query_copy().wait_recv()
            stat_copy().wait_recv()

    def far_part():
        near = to_columns(st_in[...])
        tops, sums = [], []
        for i, (h, b) in enumerate(shared):
            qt = qh[block(b), :] if h == 1 else qh0[...]
            keys = range(2 + b, 4) if h == 1 else (2,)
            tiles = [mm(qt, kx[block(n), cols(h)], NT) for n in keys]
            tiles[0] = older(tiles[0])
            top = jnp.maximum(row_max(tiles), near[i])
            tiles = expos(tiles, top)
            total = row_sum(tiles) + near[3 + i] * jnp.exp2((near[i] - top) * SOFT)
            part = weigh(tiles, total, [vx[block(n), cols(h)] for n in keys])
            scale = scale_of(part, 0)
            code = encode(part, LEVELS / scale).astype(BF16)
            scale = jnp.broadcast_to(scale, (8, FEAT)).astype(BF16)
            if h == 1:
                oc[b, pl.ds(0, BLK), :] = code
                oc[b, pl.ds(BLK, 8), :] = scale
            else:
                oc0[pl.ds(0, BLK), :] = code
                oc0[pl.ds(BLK, 8), :] = scale
            tops += halves(top)
            sums += halves(total)
        st_joint[...] = to_rows(tops + sums)[:16]

    def near_part():
        with scope("wait_o"):

            @pl.when(s > 0)
            def _():
                attn0_copy().wait_recv()
                attn_copy().wait_recv()
                total_copy().wait_recv()

        @pl.when(s == 0)
        def _():
            st_back[...] = st[...]
            oh[...] = jnp.zeros((2, BLK + 8, FEAT), BF16)
            oh0[...] = jnp.zeros((BLK + 8, FEAT), BF16)

        joint = to_columns(st_back[...])
        for i, (h, b) in enumerate(shared):
            tiles, values = near_tiles(h, b)
            near = weigh(expos(tiles, joint[i]), joint[3 + i], values)
            code = oh[b] if h == 1 else oh0[...]
            far = decode(code[:BLK], code[BLK:].astype(F32)[:1, :] * (1.0 / LEVELS))
            out[block(b), cols(h)] = near + jnp.where(s > 0, far, 0.0)

    prepare(0)
    with scope("greet"):
        pl.semaphore_wait(barrier, greeted)
    rate_load.wait()
    q_load.wait()
    for load in loads[0][3:]:
        load.wait()
    send("k", "query_leg", "query", "v_leg", "v", "query0")
    with scope("grad0"):
        gradients(0)
    prepare(1)
    with scope("grad1"):
        gradients(1)
    with scope("forward"):
        pass_on(query_leg, "query_forward")
        pass_on(v_leg, "v_forward")
    for load in late_loads:
        load.wait()
    with scope("wait_k"):

        @pl.when(s > 0)
        def _():
            k_copy().wait_recv()

        @pl.when(s == 0)
        def _():
            kh[...] = jnp.zeros((BLK, FEAT), BF16)
            vh[...] = jnp.zeros((BLK, FEAT), BF16)

    with scope("stats"):
        near_stats()
    send("stat")

    def x_sum(i):
        h, ms = GROUPS[i]
        with scope(f"wait_rx{i}"):
            received(reduce_x(i))
        steps = [rx[i, d, pl.ds(64 * len(ms), 8), :].astype(F32) * (1.0 / LEVELS) for d in range(XS - 1)]
        codes, scales = [], []
        for n, m in enumerate(ms):
            total = g[h, m, pl.ds(pl.multiple_of(x * 64, 64), 64), :]
            for d in range(XS - 1):
                total = total + decode(rx[i, d, pl.ds(64 * n, 64), :], steps[d][n : n + 1, :])
            sx[h, m] = total
            scale = scale_of(total, 0)
            scales.append(scale)
            codes.append(encode(total, LEVELS / scale).reshape(ZS, 8, FEAT))
        codes.append(jnp.broadcast_to(pick_rows(scales, (8, FEAT), 0), (ZS, 8, FEAT)))
        sc[i, :, pl.ds(0, 8 * len(ms) + 8), :] = jnp.concatenate(codes, axis=1).astype(BF16)
        start(reduce_z(i))

    mine = pl.ds(pl.multiple_of(s * 8, 8), 8)

    def renorm(i):
        h, ms = GROUPS[i]
        with scope(f"wait_rz{i}"):
            received(reduce_z(i))
        codes = [rz[i, d, pl.ds(0, 8 * len(ms) + 8), :].astype(F32) for d in range(ZS - 1)]
        parts = []
        for n, m in enumerate(ms):
            total = sx[h, m, pl.ds(pl.multiple_of(zz * 8, 8), 8), :]
            for code in codes:
                row = 8 * len(ms) + n
                total = total + decode(code[8 * n : 8 * n + 8, :], code[row : row + 1, :] * (1.0 / LEVELS))
            upd = wt[h, m, mine, :] + total
            was = old[h, m, mine, :]
            cur = jnp.sqrt(jnp.sum(upd * upd, axis=1, keepdims=True) + EPS)
            parts.append(encode_root(upd * (was / cur), was))
        nc[i, x, zz, pl.ds(0, 8 * len(ms)), :] = jnp.concatenate(parts, axis=0).astype(BF16)
        start(gather_z(i))

    def spread(i):
        with scope(f"wait_gz{i}"):
            received(gather_z(i))
        start(gather_x(i))

    def unpack(i):
        h, ms = GROUPS[i]
        with scope(f"wait_gx{i}"):
            received(gather_x(i))
        for n, m in enumerate(ms):
            fresh = decode_root(nc[i, :, :, pl.ds(8 * n, 8), :].reshape(FEAT, FEAT), old[h, m])
            hi, lo = split(fresh)
            nb[m, 0] = hi
            nb[m, 1] = lo
            g[h, m] = fresh

    def gate(h):
        unpack(2 * h)

        @pl.loop(0, TOK // BLK, unroll=True)
        def _(i):
            begin = pl.multiple_of(i * BLK, BLK)
            qt = q[pl.ds(begin, BLK), cols(h)]
            p1 = mm(qt, nb[0, 0], NT) + mm(qt, nb[0, 1], NT)
            p3 = mm(qt, nb[1, 0], NT) + mm(qt, nb[1, 1], NT)
            hi, lo = split(p1 * sigmoid(p1) * p3)
            act[0, pl.ds(begin, BLK), :] = hi
            act[1, pl.ds(begin, BLK), :] = lo

    def project(h):
        unpack(2 * h + 1)

        @pl.loop(0, TOK // BLK, unroll=True)
        def _(i):
            part = pl.ds(pl.multiple_of(i * BLK, BLK), BLK)
            hi, lo = act[0, part, :], act[1, part, :]
            o = mm(hi, nb[2, 0], NT) + mm(lo, nb[2, 0], NT) + mm(hi, nb[2, 1], NT)
            z[part, cols(h)] = o * hscale[h]

    def send_if(which, *names):
        @pl.when(which)
        def _():
            send(*names)

    x_sum(0)
    x_sum(1)
    with scope("attn02"):
        attend(0, 2)
    x_sum(2)
    x_sum(3)
    with scope("attn03"):
        attend(0, 3)
    renorm(0)
    renorm(1)
    with scope("far"):

        @pl.when(s < last)
        def _():
            await_query()
            far_part()

    send("attn_leg")
    renorm(2)
    renorm(3)
    send("total")
    send_if(me_h % 2 == 0, "attn", "attn0")
    spread(0)
    spread(1)
    with scope("attn12"):
        attend(1, 2)
    with scope("wait_v"):

        @pl.when(s > 0)
        def _():
            v_copy().wait_recv()

    with scope("attn01"):
        attend(0, 1)
    spread(2)
    spread(3)
    send_if(me_h % 2 == 1, "attn", "attn0")
    with scope("attn13"):
        attend(1, 3)
    with scope("gate0"):
        gate(0)
    with scope("project0"):
        project(0)
    with scope("forward_o"):
        pass_on(attn_leg, "attn_forward")
    with scope("gate1"):
        gate(1)
    with scope("project1"):
        project(1)

    packed = jnp.zeros((128, 128), F32)
    for r in range(TOK // 128):
        zt = z[pl.ds(r * 128, 128), :]
        packed = jnp.where(lane == r, jnp.sum(zt * zt, axis=1, keepdims=True), packed)
    sq[0] = packed.T[:8, :]
    sqs = [
        remote(sq.at[0], sq.at[d], sq_s.at[d - 1], sq_r.at[d - 1], {"head": (me_h + d) % HS})
        for d in range(1, HS)
    ]
    start(sqs)

    for h in range(2):
        for m in range(3):
            nout[m, h] = g[h, m].T

    with scope("near"):
        near_part()

    with scope("wait_sq"):
        for copy in sqs:
            copy.wait_recv()
    total = sq[0]
    for d in range(1, HS):
        total = total + sq[d]
    inv = 1.0 / jnp.sqrt(total / (2 * HS * FEAT) + EPS)
    inv_out[...] = jnp.concatenate([inv, jnp.zeros((120, 128), F32)], axis=0).T
    with scope("wait_end"):
        for i in range(4):
            for copy in reduce_x(i) + reduce_z(i) + gather_z(i) + gather_x(i):
                copy.wait_send()
        for copy in sqs:
            copy.wait_send()
        drain_halo()


def combine(attn, z, inv, fresh, mixed_hbm, n1_hbm, n3_hbm, n2_hbm, out, sem):
    copies = [
        pltpu.make_async_copy(fresh.at[m], ref, sem.at[8 + m])
        for m, ref in enumerate((n1_hbm, n3_hbm, n2_hbm))
    ]
    for copy in copies:
        copy.start()
    scale = inv[...]
    for r in range(TOK // 128):
        part = pl.ds(r * 128, 128)
        out[part, :] = attn[part, :] + z[part, :] * scale[:, r : r + 1]
        copy = pltpu.make_async_copy(out.at[part, :], mixed_hbm.at[part, :], sem.at[r])
        copy.start()
        copies.append(copy)
    for copy in copies:
        copy.wait()


def per_device(queries, keys, values, rates, head_scale, w_one, w_three, w_two):
    any_space = pl.BlockSpec(memory_space=pltpu.HBM)
    vmem = pl.BlockSpec(memory_space=pltpu.VMEM)
    dma = pltpu.SemaphoreType.DMA
    rows = jax.ShapeDtypeStruct((TOK, 2 * FEAT), F32)
    weight = jax.ShapeDtypeStruct((2, FEAT, FEAT), F32)
    pinned = [
        pltpu.with_memory_space_constraint(a, pltpu.HBM) for a in (queries, keys, values, rates.T, head_scale, w_one, w_three, w_two)
    ]
    attn, z, inv, fresh = pl.pallas_call(
        layer,
        out_shape=(rows, rows, jax.ShapeDtypeStruct((128, 128), F32), jax.ShapeDtypeStruct((3, 2, FEAT, FEAT), F32)),
        in_specs=[any_space] * 8,
        out_specs=(vmem,) * 4,
        scratch_shapes=[
            pltpu.VMEM((TOK, 2 * FEAT), BF16),
            pltpu.VMEM((TOK, 2 * FEAT), BF16),
            pltpu.VMEM((TOK, 2 * FEAT), BF16),
            pltpu.VMEM((2, TOK), F32),
            pltpu.SMEM((2,), F32),
            pltpu.VMEM((3, 2, FEAT, FEAT), F32),
            pltpu.VMEM((2, 3, FEAT, FEAT), F32),
            pltpu.VMEM((2, 3, 2, FEAT, FEAT), BF16),
            pltpu.VMEM((2, 3, FEAT, 1), F32),
            pltpu.VMEM((6, FEAT, TOK), BF16),
            pltpu.VMEM((2, 3, FEAT, FEAT), F32),
            pltpu.VMEM((4, XS, 136, FEAT), BF16),
            pltpu.VMEM((4, XS - 1, 136, FEAT), BF16),
            pltpu.VMEM((2, 3, 64, FEAT), F32),
            pltpu.VMEM((4, ZS, 24, FEAT), BF16),
            pltpu.VMEM((4, ZS - 1, 24, FEAT), BF16),
            pltpu.VMEM((4, XS, ZS, 16, FEAT), BF16),
            pltpu.VMEM((3, 2, FEAT, FEAT), BF16),
            pltpu.VMEM((2, TOK, FEAT), BF16),
            pltpu.VMEM((HS, 8, 128), F32),
            pltpu.VMEM((BLK, FEAT), BF16),
            pltpu.VMEM((BLK, FEAT), BF16),
            pltpu.VMEM((BLK, FEAT), BF16),
            pltpu.VMEM((WINDOW, FEAT), BF16),
            pltpu.VMEM((BLK, FEAT), BF16),
            pltpu.VMEM((WINDOW, FEAT), BF16),
            pltpu.VMEM((16, 128), F32),
            pltpu.VMEM((16, 128), F32),
            pltpu.VMEM((16, 128), F32),
            pltpu.VMEM((16, 128), F32),
            pltpu.VMEM((2, BLK + 8, FEAT), BF16),
            pltpu.VMEM((BLK + 8, FEAT), BF16),
            pltpu.VMEM((2, BLK + 8, FEAT), BF16),
            pltpu.VMEM((BLK + 8, FEAT), BF16),
            pltpu.VMEM((2, BLK + 8, FEAT), BF16),
            dma((14,)),
            dma((14,)),
            dma((11,)),
            dma((4, XS - 1)),
            dma((4, XS - 1)),
            dma((4, ZS - 1)),
            dma((4, ZS - 1)),
            dma((4, ZS - 1)),
            dma((4, ZS - 1)),
            dma((4, XS - 1)),
            dma((4, XS - 1)),
            dma((HS - 1,)),
            dma((HS - 1,)),
        ],
        compiler_params=pltpu.CompilerParams(
            collective_id=0, has_side_effects=True, vmem_limit_bytes=44 * 1024 * 1024
        ),
        name="layer",
    )(*pinned)
    return pl.pallas_call(
        combine,
        out_shape=(rows, weight, weight, weight),
        in_specs=[vmem] * 4,
        out_specs=(any_space,) * 4,
        scratch_shapes=[pltpu.VMEM((TOK, 2 * FEAT), F32), dma((11,))],
        compiler_params=pltpu.CompilerParams(vmem_limit_bytes=16 * 1024 * 1024),
        name="combine",
    )(attn, z, inv, fresh)


def solution(mesh):
    tile = P("seq", "head")
    weight = P("head", None, None)
    return jax.shard_map(
        per_device,
        mesh=mesh,
        in_specs=(tile, tile, tile, tile, P("head"), weight, weight, weight),
        out_specs=(tile, weight, weight, weight),
        check_vma=False,
    )
```
